32 devices in a mesh: wide: 16 (over z, y, x), narrow: 2 (over core).
Axes of the slice: x: 2, y: 2, z: 4, core: 2. Of those that a mesh axis runs over, the one named last changes fastest.
Arguments:
- tokens: bfloat16 [4096, 4096], P(('wide', 'narrow')), may hold values from -6 to 6
- expert_ids: int32 [4096, 2], P(('wide', 'narrow')), may hold values from 0 to 31, all different within a row; in each aligned block of 128 rows (0 to 127, 128 to 255, ...) at most 12 rows name the same one
- gate_values: bfloat16 [4096, 2], P(('wide', 'narrow')), may hold values from 0.099609375 to 1
- capacity: int32 [32], replicated, may hold values from 128 to 383
- w_gate: bfloat16 [32, 4096, 768], P(('wide', 'narrow')), may hold values from -0.09375 to 0.09375
- w_up: bfloat16 [32, 4096, 768], P(('wide', 'narrow')), may hold values from -0.09375 to 0.09375
- w_down: bfloat16 [32, 768, 4096], P(('wide', 'narrow')), may hold values from -0.21875 to 0.21875
Outputs:
- mixed: bfloat16 [4096, 4096], P(('wide', 'narrow'))
The draws below stay inside these ranges and needn't reach their ends.
Inputs may be any that keep to these rules, and one draw needn't show every extreme that they name: `expert_ids`: the two experts of a token differ; among the tokens of one device no expert is named more than 12 times, and that many is reached.
All inputs are finite; a program needn't handle non-finite values.
Results may differ from the reference program's by a relative error of at most 0.0058.
Values may be sent and summed in bfloat16 or wider, within the bound.
A program may use at most 128 MiB of HBM per device.

```python
import math
import jax
import jax.numpy as jnp
import numpy as np
from jax import lax

D = 4096
FF = 768
TOK_DEV = 128
TOKENS = 4096
EXPERTS = 32
MOST = 12


def with_ends(array, rng, least, largest):
    dims = array.shape
    place = [jax.random.randint(jax.random.fold_in(rng, axis), (), 0, dims[axis]) for axis in range(len(dims))]
    array = array.at[tuple(place)].set(least)
    longest = dims.index(max(dims))
    place[longest] = (place[longest] + 1) % dims[longest]
    return array.at[tuple(place)].set(largest)


def block_levels(stream_key, dims, pieces, low, high):
    factor_of = 1.0
    for dim, blocks in pieces:
        heights = jax.random.uniform(jax.random.fold_in(jax.random.fold_in(stream_key, 6), dim), (blocks,), jnp.float32, low / len(pieces), high / len(pieces))
        factor_of = factor_of * jnp.repeat(jnp.exp(heights), dims[dim] // blocks).reshape((-1,) + (1,) * (len(dims) - 1 - dim))
    return factor_of


def deal_out(own_key, own, number, rows, amount, top, bound, slope):
    order = jax.random.permutation(own_key, amount)
    packed, common = load_shares(amount, rows * top, bound, slope, True), load_shares(amount, rows * top, bound, slope, False)
    places = jnp.arange(amount)

    def named(tallies, turn):
        used = int((tallies > 0).sum())
        fixed = max(1, used // 4)
        passed = fixed + (places - fixed + turn * (used - fixed)) % max(1, amount - fixed)
        return jnp.zeros((amount,), jnp.int32).at[order[jnp.where(places < fixed, places, passed)]].set(jnp.asarray(tallies, jnp.int32))

    tallies = jnp.where(number % 4 == 0, named(packed, number // 4), named(common, number - number // 4 - 1))
    mixed = jax.random.permutation(jax.random.fold_in(own, 3), amount)
    donor, taker = mixed[0:amount // 2 * 2:2], mixed[1:amount // 2 * 2:2]
    slack = jnp.minimum(tallies[donor] - 1, bound - tallies[taker]) // 2
    slack = jnp.where((donor == order[0]) | (taker == order[0]) | (tallies[taker] == 0), 0, jnp.maximum(slack, 0))
    passed = jax.random.randint(jax.random.fold_in(own, 4), (amount // 2,), 0, 1 << 20) % (slack + 1)
    tallies = tallies.at[donor].add(-passed).at[taker].add(passed)
    labels = jnp.searchsorted(jnp.cumsum(tallies), jnp.arange(rows * top), side="right").astype(jnp.int32)
    listing = labels.reshape(top, rows).T
    listing = listing[jax.random.permutation(jax.random.fold_in(own, 1), rows)]
    turn = jax.random.randint(jax.random.fold_in(own, 2), (rows, 1), 0, top)
    return jnp.take_along_axis(listing, (jnp.arange(top)[None, :] + turn) % top, axis=1)


def load_shares(amount, total, reach, skew, full):
    loads = [(1 << 20) // math.isqrt(standing ** skew) + 1 for standing in range(1, amount + 1)]
    largest = reach if full else min(reach, max(-(-total // amount), total * loads[0] // sum(loads)))
    least = 1 if total - largest >= amount - 1 else 0
    counts, rest = [largest] + [least] * (amount - 1), total - largest - least * (amount - 1)
    while rest > 0:
        candidates = [i for i in range(1, amount) if counts[i] < largest] or [i for i in range(1, amount) if counts[i] < reach]
        whole, remaining = sum([loads[i] for i in candidates]), rest
        for i in candidates:
            addition = min(reach - counts[i], max(1, remaining * loads[i] // whole), rest)
            counts[i] = counts[i] + addition
            rest = rest - addition
    return np.array(counts)


def normal_values(key, extent, scale, limit, shards=(), kind=jnp.bfloat16):
    array = jax.random.normal(key, extent, jnp.float32) * scale
    if len(shards) > 0:
        array = block_levels(key, extent, shards, -0.22, 0.18) * array
    return jnp.clip(array, min=-limit, max=limit).astype(kind)


def setup_inputs(seed: int = 0) -> dict:
    splits = jax.random.split(jax.random.key(seed), 8)
    tokens = normal_values(splits[0], (TOKENS, D), 1.0, 6.0, ((0, 32),))
    expert_ids_keys = jax.random.split(jax.random.fold_in(splits[1], 1), TOKENS // TOK_DEV)
    expert_ids_turns = jax.random.permutation(jax.random.fold_in(splits[1], 3), TOKENS // TOK_DEV)
    expert_ids = jax.vmap(lambda own, number: deal_out(jax.random.fold_in(splits[1], 2), own, number, TOK_DEV, EXPERTS, 2, MOST, 2))(expert_ids_keys, expert_ids_turns).reshape((TOKENS, 2))
    gate_values = jnp.clip(0.099609375 + 0.9003906 * jax.random.uniform(splits[2], (TOKENS, 2), jnp.float32) ** block_levels(splits[2], (TOKENS, 2), ((0, 32),), -0.2, 0.2), 0.099609375, 1.0).astype(jnp.bfloat16)
    capacity = with_ends(jax.random.randint(splits[3], (EXPERTS,), TOK_DEV, 3 * TOK_DEV), jax.random.fold_in(splits[3], 1), TOK_DEV, (3 * TOK_DEV) - 1).astype(jnp.int32)
    w_gate = normal_values(splits[4], (EXPERTS, D, FF), D ** -0.5, 0.09375, ((0, 32),))
    w_up = normal_values(splits[5], (EXPERTS, D, FF), D ** -0.5, 0.09375, ((0, 32),))
    w_down = normal_values(splits[6], (EXPERTS, FF, D), FF ** -0.5, 0.21875, ((0, 32),))
    return {"tokens": tokens, "expert_ids": expert_ids, "gate_values": gate_values, "capacity": capacity, "w_gate": w_gate, "w_up": w_up, "w_down": w_down}


def expert_apply(token_rows, gate_matrix, up_matrix, down_matrix):
    gate_part = jnp.dot(token_rows, gate_matrix, preferred_element_type=jnp.float32)
    up_part = jnp.dot(token_rows, up_matrix, preferred_element_type=jnp.float32)
    hidden = (jax.nn.silu(gate_part) * up_part).astype(jnp.bfloat16)
    return jnp.dot(hidden, down_matrix, preferred_element_type=jnp.float32).astype(jnp.bfloat16)


def reference(tokens, expert_ids, gate_values, capacity, w_gate, w_up, w_down):
    assigns = 2 * TOKENS
    flat_ids = expert_ids.reshape(-1).astype(jnp.int32)
    onehot = (flat_ids[:, None] == jnp.arange(EXPERTS, dtype=jnp.int32)[None, :]).astype(jnp.int32)
    global_rank = jnp.sum((jnp.cumsum(onehot, axis=0) - onehot) * onehot, axis=1).astype(jnp.int32)
    kept_mask = global_rank < capacity[flat_ids]
    room_rows = 3 * TOK_DEV
    slot_index = jnp.where(kept_mask, global_rank, room_rows).astype(jnp.int32)
    table = jnp.full((EXPERTS, room_rows + 1), assigns, jnp.int32)
    table = table.at[flat_ids, slot_index].set(jnp.arange(assigns, dtype=jnp.int32))
    table = table[:, :room_rows]
    weights = gate_values.reshape(-1).astype(jnp.float32) * kept_mask.astype(jnp.float32)
    padded_weights = jnp.concatenate([weights, jnp.zeros((1,), jnp.float32)])
    padded_tokens = jnp.concatenate([tokens, jnp.zeros((1, D), jnp.bfloat16)], axis=0)

    def expert_step(summed, inputs):
        column, gate_matrix, up_matrix, down_matrix = inputs
        owners = (column // 2).astype(jnp.int32)
        token_rows = padded_tokens[owners]
        results = expert_apply(token_rows, gate_matrix, up_matrix, down_matrix)
        scaled = results.astype(jnp.float32) * padded_weights[column][:, None]
        return summed.at[owners].add(scaled), None

    start = jnp.zeros((TOKENS + 1, D), jnp.float32)
    summed, unused = lax.scan(expert_step, start, (table, w_gate, w_up, w_down))
    return summed[:TOKENS].astype(jnp.bfloat16)
```

```python
import functools
import math

import jax
import jax.numpy as jnp
import numpy as np
from jax import lax
from jax.experimental import pallas as pl
from jax.experimental.pallas import tpu as pltpu
from jax.sharding import PartitionSpec as P

MESH = pl.DeviceIdType.MESH
PIECES = 16
F32 = jnp.float32
BF16 = jnp.bfloat16


def flip(me, off, bits):
    out = 0
    for b in range(bits):
        w = 1 << b
        out = out + (((me // w) % 2 + (off // w) % 2) % 2) * w
    return out


def alternate(k, groups):
    return (k % 2) * (groups - 1 - k // 2) + (1 - k % 2) * (k // 2)


def kernel(n, narrow, most, unit, tok, put, mix, pick, counts, cap, rank, row_mask, col_mask, gather, spread,
           wg_hbm, wu_hbm, wd_hbm, out,
           wg, wu, wd, sent, came, back, home, x, y, total, seen,
           s1, r1, s2, r2, s3, r3, wsem):
    bits = int(math.log2(n))
    groups = n // unit
    rows = unit * unit * most
    part = unit * most
    width = tok.shape[1]
    piece = width // PIECES
    quads = PIECES // unit
    me = lax.axis_index("wide") * narrow + lax.axis_index("narrow")

    def where_is(off):
        peer = flip(me, off, bits)
        return (peer // narrow, peer % narrow)

    loads = [
        pltpu.make_async_copy(h.at[0], v, wsem.at[i])
        for i, (h, v) in enumerate(((wg_hbm, wg), (wu_hbm, wu), (wd_hbm, wd)))
    ]
    for load in loads:
        load.start()

    barrier = pltpu.get_barrier_semaphore()

    @pl.loop(1, n)
    def _(off):
        pl.semaphore_signal(barrier, inc=1, device_id=where_is(off), device_id_type=MESH)

    pl.semaphore_wait(barrier, n - 1)

    def count_copy(off):
        return pltpu.make_async_remote_copy(
            src_ref=counts, dst_ref=seen.at[off], send_sem=s3.at[off], recv_sem=r3.at[off],
            device_id=where_is(off), device_id_type=MESH)

    def out_copy(off):
        return pltpu.make_async_remote_copy(
            src_ref=sent.at[off], dst_ref=came.at[off], send_sem=s1.at[off], recv_sem=r1.at[off],
            device_id=where_is(off), device_id_type=MESH)

    def back_copy(off):
        return pltpu.make_async_remote_copy(
            src_ref=back.at[off], dst_ref=home.at[off], send_sem=s2.at[off], recv_sem=r2.at[off],
            device_id=where_is(off), device_id_type=MESH)

    def each_remote(g, act):
        for i in range(unit):
            off = g * unit + i
            if i:
                act(off)
            else:
                @pl.when(g > 0)
                def _(off=off):
                    act(off)

    @pl.loop(0, groups)
    def _(k):
        g = (groups - 1) * ((k + 1) % 2) - (k // 2) * ((k + 1) % 2) + (k // 2) * (k % 2)
        onehot = put[g]
        masked = [onehot * row_mask[j] for j in range(unit)]
        for q in range(quads):
            acc = jnp.zeros((rows, piece), F32)
            for j in range(unit):
                at = (q * unit + j) * piece
                acc = acc + jnp.dot(masked[j], tok[:, at:at + piece], preferred_element_type=F32)
            block = acc.astype(BF16).reshape(unit, part, piece)
            sent[pl.ds(g * unit, unit), q * part:(q + 1) * part, :] = block
        each_remote(g, lambda off: out_copy(off).start())

        @pl.when(g == 0)
        def _():
            came[0] = sent[0]

    @pl.loop(1, n)
    def _(off):
        count_copy(off).start()

    for load in loads:
        load.wait()

    @pl.loop(0, groups)
    def _(k):
        g = alternate(k, groups)
        each_remote(g, lambda off: out_copy(off).wait_recv())
        for q in range(quads):
            block = came[pl.ds(g * unit, unit), q * part:(q + 1) * part, :].reshape(rows, piece)
            for j in range(unit):
                at = (q * unit + j) * piece
                x[:, at:at + piece] = jnp.dot(gather[j], block, preferred_element_type=F32).astype(BF16)
        xs = x[...]
        gate = jnp.dot(xs, wg[...], preferred_element_type=F32)
        up = jnp.dot(xs, wu[...], preferred_element_type=F32)
        hidden = (gate / (1.0 + jnp.exp(-gate)) * up).astype(BF16)
        y[...] = jnp.dot(hidden, wd[...], preferred_element_type=F32).astype(BF16)
        for q in range(quads):
            acc = jnp.zeros((rows, piece), F32)
            for j in range(unit):
                at = (q * unit + j) * piece
                acc = acc + jnp.dot(spread[j], y[:, at:at + piece], preferred_element_type=F32)
            block = acc.astype(BF16).reshape(unit, part, piece)
            back[pl.ds(g * unit, unit), q * part:(q + 1) * part, :] = block
        each_remote(g, lambda off: back_copy(off).start())

        @pl.when(g == 0)
        def _():
            home[0] = back[0]

    seen[0] = jnp.zeros_like(seen[0])

    @pl.loop(1, n)
    def _(off):
        count_copy(off).wait()

    def earlier(off, tally):
        ahead = jnp.where(flip(me, off, bits) < me, 1, 0)
        return tally + seen[off] * ahead

    before = lax.fori_loop(1, n, earlier, jnp.zeros(counts.shape, jnp.int32))
    left = jnp.clip(cap[...] - before, 0, most).astype(F32).astype(BF16)

    total[...] = jnp.zeros_like(total)

    @pl.loop(0, groups)
    def _(k):
        g = alternate(k, groups)
        room = jnp.dot(left, pick[g], preferred_element_type=F32)[0:1, :]
        kept = jnp.where(room > rank[...], 1.0, 0.0).astype(BF16)
        weights = mix[g] * kept
        masked = [weights * col_mask[j] for j in range(unit)]
        each_remote(g, lambda off: back_copy(off).wait_recv())
        for q in range(quads):
            block = home[pl.ds(g * unit, unit), q * part:(q + 1) * part, :].reshape(rows, piece)
            for j in range(unit):
                at = (q * unit + j) * piece
                total[:, at:at + piece] += jnp.dot(masked[j], block, preferred_element_type=F32)

    out[...] = total[...].astype(BF16)

    @pl.loop(1, n)
    def _(off):
        out_copy(off).wait_send()
        back_copy(off).wait_send()


def on_device(n, narrow, tokens, expert_ids, gate_values, capacity, w_gate, w_up, w_down):
    experts = capacity.shape[0]
    tok_rows, width = tokens.shape
    hidden = w_gate.shape[2]
    most = 3 * tok_rows // experts
    unit = 16 // math.gcd(16, most)
    groups = n // unit
    rows = unit * unit * most
    me = lax.axis_index("wide") * narrow + lax.axis_index("narrow")
    me = me.astype(jnp.int32)

    flat = expert_ids.reshape(-1)
    onehot = (flat[:, None] == jnp.arange(experts, dtype=jnp.int32)[None, :]).astype(BF16)
    triangle = jnp.asarray(np.tril(np.ones((2 * tok_rows,) * 2), -1), BF16)
    before = jnp.dot(triangle, onehot, preferred_element_type=F32)
    rank = jnp.sum(before * onehot.astype(F32), axis=1).astype(jnp.int32)
    tally = jnp.sum(onehot.astype(F32), axis=0).astype(jnp.int32)
    lanes = -(-experts // 128) * 128
    counts = jnp.broadcast_to(jnp.pad(tally, (0, lanes - experts))[None], (8, lanes))
    cap = jnp.broadcast_to(jnp.pad(capacity, (0, lanes - experts))[None], (8, lanes))
    slot = ((flat ^ me) * most + rank).reshape(tok_rows, 2)

    i, j, r = np.meshgrid(np.arange(unit), np.arange(unit), np.arange(most), indexing="ij")
    i, j, r = i.reshape(-1), j.reshape(-1), r.reshape(-1)
    code = (np.arange(groups)[:, None] * unit + i[None]) * most + r[None]
    partner = np.arange(groups)[:, None] * unit + i[None]
    code, partner = jnp.asarray(code, jnp.int32), jnp.asarray(partner, jnp.int32)
    hit = [slot[:, c][None, :] == code[:, :, None] for c in (0, 1)]
    put = (hit[0] | hit[1]).astype(BF16)
    mix = sum(
        jnp.where(slot[:, c][None, :, None] == code[:, None, :], gate_values[:, c][None, :, None], 0)
        for c in (0, 1)
    ).astype(BF16)
    pick = (jnp.arange(lanes, dtype=jnp.int32)[None, :, None] == (partner ^ me)[:, None, :]).astype(BF16)
    rank_row = jnp.asarray(r[None], F32)
    which = np.arange(unit)
    row_mask = jnp.asarray(np.broadcast_to((j[None] == which[:, None])[:, :, None], (unit, rows, tok_rows)), BF16)
    col_mask = jnp.asarray((j[None] == which[:, None])[:, None, :], BF16)
    short = np.arange(unit * most)
    gather = (short[None, :, None] == (i * most + r)[None, None, :]) & (j[None] == which[:, None])[:, None, :]
    gather, spread = jnp.asarray(gather, BF16), jnp.asarray(gather.transpose(0, 2, 1), BF16)

    block = (PIECES * most, width // PIECES)
    vmem = pl.BlockSpec(memory_space=pltpu.VMEM)
    hbm = pl.BlockSpec(memory_space=pl.ANY)
    dma = pltpu.SemaphoreType.DMA
    return pl.pallas_call(
        functools.partial(kernel, n, narrow, most, unit),
        out_shape=jax.ShapeDtypeStruct((tok_rows, width), BF16),
        in_specs=[vmem] * 11 + [hbm] * 3,
        out_specs=vmem,
        scratch_shapes=[
            pltpu.VMEM((width, hidden), BF16),
            pltpu.VMEM((width, hidden), BF16),
            pltpu.VMEM((hidden, width), BF16),
            pltpu.VMEM((n,) + block, BF16),
            pltpu.VMEM((n,) + block, BF16),
            pltpu.VMEM((n,) + block, BF16),
            pltpu.VMEM((n,) + block, BF16),
            pltpu.VMEM((unit * most, width), BF16),
            pltpu.VMEM((unit * most, width), BF16),
            pltpu.VMEM((tok_rows, width), F32),
            pltpu.VMEM((n, 8, lanes), jnp.int32),
            dma((n,)), dma((n,)), dma((n,)), dma((n,)), dma((n,)), dma((n,)), dma((3,)),
        ],
        compiler_params=pltpu.CompilerParams(
            collective_id=0, has_side_effects=True, vmem_limit_bytes=60 * 1024 * 1024
        ),
    )(tokens, put, mix, pick, counts, cap, rank_row, row_mask, col_mask, gather, spread, w_gate, w_up, w_down)


def solution(mesh):
    both = ("wide", "narrow")
    n, narrow = mesh.shape["wide"] * mesh.shape["narrow"], mesh.shape["narrow"]
    return jax.shard_map(
        functools.partial(on_device, n, narrow),
        mesh=mesh,
        in_specs=(P(both, None), P(both, None), P(both, None), P(),
                  P(both, None, None), P(both, None, None), P(both, None, None)),
        out_specs=P(both, None),
        check_vma=False,
    )
```

```python
import functools
import math

import jax
import jax.numpy as jnp
import numpy as np
from jax import lax
from jax.experimental import pallas as pl
from jax.experimental.pallas import tpu as pltpu
from jax.sharding import PartitionSpec as P

MESH = pl.DeviceIdType.MESH
PIECES = 16
F32 = jnp.float32
BF16 = jnp.bfloat16


def flip(me, off, bits):
    out = 0
    for b in range(bits):
        w = 1 << b
        out = out + (((me // w) % 2 + (off // w) % 2) % 2) * w
    return out


def orders(groups):
    if groups != 8:
        return None
    return [sum(g * 8**k for k, g in enumerate(o)) for o in ((7, 0, 1, 2, 6, 3, 5, 4), (0, 1, 7, 2, 6, 3, 5, 4))]


def in_order(groups, which, body):
    if orders(groups) is None:
        def plain(k, carry):
            body(k)
            return carry
        lax.fori_loop(0, groups, plain, 0)
        return

    def step(k, digits):
        body(digits % groups)
        return digits // groups

    lax.fori_loop(0, groups, step, jnp.int32(orders(groups)[which]))


def kernel(n, narrow, most, unit, tok, put, mix, pick, counts, cap, rank, row_mask, col_mask, gather, spread,
           wg_hbm, wu_hbm, wd_hbm, out,
           wg, wu, wd, sent, came, back, home, x, y, total, seen,
           s1, r1, s2, r2, s3, r3, wsem):
    bits = int(math.log2(n))
    groups = n // unit
    rows = unit * unit * most
    part = unit * most
    width = tok.shape[1]
    piece = width // PIECES
    quads = PIECES // unit
    me = lax.axis_index("wide") * narrow + lax.axis_index("narrow")

    def where_is(off):
        peer = flip(me, off, bits)
        return (peer // narrow, peer % narrow)

    loads = [
        pltpu.make_async_copy(h.at[0], v, wsem.at[i])
        for i, (h, v) in enumerate(((wg_hbm, wg), (wu_hbm, wu), (wd_hbm, wd)))
    ]
    for load in loads:
        load.start()

    barrier = pltpu.get_barrier_semaphore()

    @pl.loop(1, n)
    def _(off):
        pl.semaphore_signal(barrier, inc=1, device_id=where_is(off), device_id_type=MESH)

    pl.semaphore_wait(barrier, n - 1)

    def count_copy(off):
        return pltpu.make_async_remote_copy(
            src_ref=counts, dst_ref=seen.at[off], send_sem=s3.at[off], recv_sem=r3.at[off],
            device_id=where_is(off), device_id_type=MESH)

    def out_copy(off):
        return pltpu.make_async_remote_copy(
            src_ref=sent.at[off], dst_ref=came.at[off], send_sem=s1.at[off], recv_sem=r1.at[off],
            device_id=where_is(off), device_id_type=MESH)

    def back_copy(off):
        return pltpu.make_async_remote_copy(
            src_ref=back.at[off], dst_ref=home.at[off], send_sem=s2.at[off], recv_sem=r2.at[off],
            device_id=where_is(off), device_id_type=MESH)

    def each_remote(g, act):
        for i in range(unit):
            off = g * unit + i
            if i:
                act(off)
            else:
                @pl.when(g > 0)
                def _(off=off):
                    act(off)

    def dispatch(g):
        onehot = put[g]
        masked = [onehot * row_mask[j] for j in range(unit)]
        for q in range(quads):
            acc = jnp.zeros((rows, piece), F32)
            for j in range(unit):
                at = (q * unit + j) * piece
                acc = acc + jnp.dot(masked[j], tok[:, at:at + piece], preferred_element_type=F32)
            block = acc.astype(BF16).reshape(unit, part, piece)
            sent[pl.ds(g * unit, unit), q * part:(q + 1) * part, :] = block
        each_remote(g, lambda off: out_copy(off).start())

        @pl.when(g == 0)
        def _():
            came[0] = sent[0]

    in_order(groups, 0, dispatch)

    @pl.loop(1, n)
    def _(off):
        count_copy(off).start()

    for load in loads:
        load.wait()

    def expert(g):
        each_remote(g, lambda off: out_copy(off).wait_recv())
        for q in range(quads):
            block = came[pl.ds(g * unit, unit), q * part:(q + 1) * part, :].reshape(rows, piece)
            for j in range(unit):
                at = (q * unit + j) * piece
                x[:, at:at + piece] = jnp.dot(gather[j], block, preferred_element_type=F32).astype(BF16)
        xs = x[...]
        gate = jnp.dot(xs, wg[...], preferred_element_type=F32)
        up = jnp.dot(xs, wu[...], preferred_element_type=F32)
        hidden = (gate / (1.0 + jnp.exp(-gate)) * up).astype(BF16)
        y[...] = jnp.dot(hidden, wd[...], preferred_element_type=F32).astype(BF16)
        for q in range(quads):
            acc = jnp.zeros((rows, piece), F32)
            for j in range(unit):
                at = (q * unit + j) * piece
                acc = acc + jnp.dot(spread[j], y[:, at:at + piece], preferred_element_type=F32)
            block = acc.astype(BF16).reshape(unit, part, piece)
            back[pl.ds(g * unit, unit), q * part:(q + 1) * part, :] = block
        each_remote(g, lambda off: back_copy(off).start())

        @pl.when(g == 0)
        def _():
            home[0] = back[0]

    in_order(groups, 1, expert)

    seen[0] = jnp.zeros_like(seen[0])

    @pl.loop(1, n)
    def _(off):
        count_copy(off).wait()

    def earlier(off, tally):
        ahead = jnp.where(flip(me, off, bits) < me, 1, 0)
        return tally + seen[off] * ahead

    before = lax.fori_loop(1, n, earlier, jnp.zeros(counts.shape, jnp.int32))
    left = jnp.clip(cap[...] - before, 0, most).astype(F32).astype(BF16)

    total[...] = jnp.zeros_like(total)

    def combine(g):
        room = jnp.dot(left, pick[g], preferred_element_type=F32)[0:1, :]
        kept = jnp.where(room > rank[...], 1.0, 0.0).astype(BF16)
        weights = mix[g] * kept
        masked = [weights * col_mask[j] for j in range(unit)]
        each_remote(g, lambda off: back_copy(off).wait_recv())
        for q in range(quads):
            block = home[pl.ds(g * unit, unit), q * part:(q + 1) * part, :].reshape(rows, piece)
            for j in range(unit):
                at = (q * unit + j) * piece
                total[:, at:at + piece] += jnp.dot(masked[j], block, preferred_element_type=F32)

    in_order(groups, 1, combine)

    out[...] = total[...].astype(BF16)

    @pl.loop(1, n)
    def _(off):
        out_copy(off).wait_send()
        back_copy(off).wait_send()


def on_device(n, narrow, tokens, expert_ids, gate_values, capacity, w_gate, w_up, w_down):
    experts = capacity.shape[0]
    tok_rows, width = tokens.shape
    hidden = w_gate.shape[2]
    most = 3 * tok_rows // experts
    unit = 16 // math.gcd(16, most)
    groups = n // unit
    rows = unit * unit * most
    me = lax.axis_index("wide") * narrow + lax.axis_index("narrow")
    me = me.astype(jnp.int32)

    flat = expert_ids.reshape(-1)
    onehot = (flat[:, None] == jnp.arange(experts, dtype=jnp.int32)[None, :]).astype(BF16)
    triangle = jnp.asarray(np.tril(np.ones((2 * tok_rows,) * 2), -1), BF16)
    before = jnp.dot(triangle, onehot, preferred_element_type=F32)
    rank = jnp.sum(before * onehot.astype(F32), axis=1).astype(jnp.int32)
    tally = jnp.sum(onehot.astype(F32), axis=0).astype(jnp.int32)
    lanes = -(-experts // 128) * 128
    counts = jnp.broadcast_to(jnp.pad(tally, (0, lanes - experts))[None], (8, lanes))
    cap = jnp.broadcast_to(jnp.pad(capacity, (0, lanes - experts))[None], (8, lanes))
    slot = ((flat ^ me) * most + rank).reshape(tok_rows, 2)

    i, j, r = np.meshgrid(np.arange(unit), np.arange(unit), np.arange(most), indexing="ij")
    i, j, r = i.reshape(-1), j.reshape(-1), r.reshape(-1)
    code = (np.arange(groups)[:, None] * unit + i[None]) * most + r[None]
    partner = np.arange(groups)[:, None] * unit + i[None]
    code, partner = jnp.asarray(code, jnp.int32), jnp.asarray(partner, jnp.int32)
    hit = [slot[:, c][None, :] == code[:, :, None] for c in (0, 1)]
    put = (hit[0] | hit[1]).astype(BF16)
    mix = sum(
        jnp.where(slot[:, c][None, :, None] == code[:, None, :], gate_values[:, c][None, :, None], 0)
        for c in (0, 1)
    ).astype(BF16)
    pick = (jnp.arange(lanes, dtype=jnp.int32)[None, :, None] == (partner ^ me)[:, None, :]).astype(BF16)
    rank_row = jnp.asarray(r[None], F32)
    which = np.arange(unit)
    row_mask = jnp.asarray(np.broadcast_to((j[None] == which[:, None])[:, :, None], (unit, rows, tok_rows)), BF16)
    col_mask = jnp.asarray((j[None] == which[:, None])[:, None, :], BF16)
    short = np.arange(unit * most)
    gather = (short[None, :, None] == (i * most + r)[None, None, :]) & (j[None] == which[:, None])[:, None, :]
    gather, spread = jnp.asarray(gather, BF16), jnp.asarray(gather.transpose(0, 2, 1), BF16)

    block = (PIECES * most, width // PIECES)
    vmem = pl.BlockSpec(memory_space=pltpu.VMEM)
    hbm = pl.BlockSpec(memory_space=pl.ANY)
    dma = pltpu.SemaphoreType.DMA
    return pl.pallas_call(
        functools.partial(kernel, n, narrow, most, unit),
        out_shape=jax.ShapeDtypeStruct((tok_rows, width), BF16),
        in_specs=[vmem] * 11 + [hbm] * 3,
        out_specs=vmem,
        scratch_shapes=[
            pltpu.VMEM((width, hidden), BF16),
            pltpu.VMEM((width, hidden), BF16),
            pltpu.VMEM((hidden, width), BF16),
            pltpu.VMEM((n,) + block, BF16),
            pltpu.VMEM((n,) + block, BF16),
            pltpu.VMEM((n,) + block, BF16),
            pltpu.VMEM((n,) + block, BF16),
            pltpu.VMEM((unit * most, width), BF16),
            pltpu.VMEM((unit * most, width), BF16),
            pltpu.VMEM((tok_rows, width), F32),
            pltpu.VMEM((n, 8, lanes), jnp.int32),
            dma((n,)), dma((n,)), dma((n,)), dma((n,)), dma((n,)), dma((n,)), dma((3,)),
        ],
        compiler_params=pltpu.CompilerParams(
            collective_id=0, has_side_effects=True, vmem_limit_bytes=60 * 1024 * 1024
        ),
    )(tokens, put, mix, pick, counts, cap, rank_row, row_mask, col_mask, gather, spread, w_gate, w_up, w_down)


def solution(mesh):
    both = ("wide", "narrow")
    n, narrow = mesh.shape["wide"] * mesh.shape["narrow"], mesh.shape["narrow"]
    return jax.shard_map(
        functools.partial(on_device, n, narrow),
        mesh=mesh,
        in_specs=(P(both, None), P(both, None), P(both, None), P(),
                  P(both, None, None), P(both, None, None), P(both, None, None)),
        out_specs=P(both, None),
        check_vma=False,
    )
```
